64 devices in a mesh: dp: 4 (over x, y), tp: 16 (over z, core).
Axes of the slice: x: 2, y: 2, z: 8, core: 2. Of those that a mesh axis runs over, the one named last changes fastest.
The devices are a block of a 4x4x8 slice.
Arguments:
- hidden: bfloat16 [32, 32, 4096], P('dp'), parts along dimension 0
- tree_mask: int32 [32, 32, 32], P('dp'), parts along dimension 0
- depth: int32 [32, 32], P('dp'), parts along dimension 0
- ctx_len: int32 [32], P('dp'), parts along dimension 0
- block_table: int32 [32, 16], P('dp'), parts along dimension 0
- score_id: int32 [32, 32], P('dp'), parts along dimension 0
- k_cache: bfloat16 [512, 16, 32, 128], P('dp', None, 'tp'), parts along dimension 0
- v_cache: bfloat16 [512, 16, 32, 128], P('dp', None, 'tp'), parts along dimension 0
- attn_norm: bfloat16 [4096], replicated
- w_q: bfloat16 [4096, 4096], P(None, 'tp')
- w_k: bfloat16 [4096, 4096], P(None, 'tp')
- w_v: bfloat16 [4096, 4096], P(None, 'tp')
- w_o: bfloat16 [4096, 4096], P('tp')
- mlp_norm: bfloat16 [4096], replicated
- w_gate: bfloat16 [4096, 11008], P(None, 'tp')
- w_up: bfloat16 [4096, 11008], P(None, 'tp')
- w_down: bfloat16 [11008, 4096], P('tp')
- final_norm: bfloat16 [4096], replicated
- w_lm: bfloat16 [4096, 102400], P(None, 'tp')
Outputs:
- output 1: float32 [32, 32], P('dp'), parts along dimension 0
- output 2: float32 [32, 32], P('dp'), parts along dimension 0
- output 3: bfloat16 [512, 16, 32, 128], P('dp', None, 'tp'), parts along dimension 0
- output 4: bfloat16 [512, 16, 32, 128], P('dp', None, 'tp'), parts along dimension 0
There are 4 independent parts. The reference program is written for one: setup_inputs(seed, part) draws one part's arguments, and reference() takes and returns one part's arrays. A program takes and returns all parts, laid end to end along the dimension named above; an argument that names none is the same for every part.
All inputs are finite; a program needn't handle non-finite values.
Results may differ from the reference program's by a relative error of at most 0.0040011.
Values are sent between devices in bfloat16 or wider.
A program may use at most 768 MiB of HBM per device.

```python
import math
import jax
import jax.numpy as jnp
from jax import lax

REQUESTS = 8
NODES = 32
PAGES = 16
PAGE_SIZE = 16
MODEL_DIM = 4096
HEADS = 32
KV_HEADS = 32
HEAD_DIM = 128
FFN_DIM = 11008
VOCAB_SIZE = 102400
ROPE_THETA = 500000
RMS_EPS = 1e-5
BLOCKS = REQUESTS * PAGES
SPAN = PAGES * PAGE_SIZE
MAX_CTX = SPAN - NODES
GROUP = HEADS // KV_HEADS


def draw_routing(key):
    k_spread, k_step, k_ctx, k_table, k_score = jax.random.split(key, 5)
    spread = jax.random.randint(k_spread, (REQUESTS, 1), 1, 4)
    step = jnp.minimum(jax.random.randint(k_step, (REQUESTS, NODES), 0, 4), spread)
    node_ids = jnp.arange(NODES)
    parent = jnp.maximum(node_ids[None, :] - 1 - step, 0)
    linked = (parent[:, :, None] == node_ids[None, None, :]) & (node_ids[None, :, None] > 0)
    reach = linked | (node_ids[:, None] == node_ids[None, :])[None]
    for _ in range(int(math.log2(NODES)) + 1):
        reach = jnp.any(reach[:, :, :, None] & reach[:, None, :, :], axis=2)
    tree_mask = reach.astype(jnp.int32)
    depth = jnp.sum(tree_mask, axis=-1).astype(jnp.int32) - 1
    ctx_len = jax.random.randint(k_ctx, (REQUESTS,), 1, MAX_CTX + 1).astype(jnp.int32)
    ctx_len = ctx_len.at[0].set(MAX_CTX)
    block_table = jax.random.permutation(k_table, BLOCKS).astype(jnp.int32).reshape(REQUESTS, PAGES)
    score_id = jax.random.randint(k_score, (REQUESTS, NODES), 0, VOCAB_SIZE).astype(jnp.int32)
    score_id = score_id.at[0, 0].set(VOCAB_SIZE - 1)
    return tree_mask, depth, ctx_len, block_table, score_id


def normal_weight(key, shape, scale):
    return (scale * jax.random.normal(key, shape, jnp.float32)).astype(jnp.bfloat16)


def gain_vector(key):
    return (1.0 + 0.3 * jax.random.normal(key, (MODEL_DIM,), jnp.float32)).astype(jnp.bfloat16)


def setup_inputs(seed: int = 0, part: int = 0) -> dict:
    part_key = jax.random.fold_in(jax.random.key(seed), part)
    keys = jax.random.split(part_key, 4)
    tree_mask, depth, ctx_len, block_table, score_id = draw_routing(keys[0])
    shared = jax.random.split(jax.random.key(seed + 1), 11)
    cache_shape = (BLOCKS, PAGE_SIZE, KV_HEADS, HEAD_DIM)
    return {
        "hidden": normal_weight(keys[1], (REQUESTS, NODES, MODEL_DIM), 1.0),
        "tree_mask": tree_mask,
        "depth": depth,
        "ctx_len": ctx_len,
        "block_table": block_table,
        "score_id": score_id,
        "k_cache": normal_weight(keys[2], cache_shape, 1.0),
        "v_cache": normal_weight(keys[3], cache_shape, 1.0),
        "attn_norm": gain_vector(shared[0]),
        "w_q": normal_weight(shared[1], (MODEL_DIM, HEADS * HEAD_DIM), 2.5 * MODEL_DIM ** -0.5),
        "w_k": normal_weight(shared[2], (MODEL_DIM, KV_HEADS * HEAD_DIM), 1.5 * MODEL_DIM ** -0.5),
        "w_v": normal_weight(shared[3], (MODEL_DIM, KV_HEADS * HEAD_DIM), MODEL_DIM ** -0.5),
        "w_o": normal_weight(shared[4], (HEADS * HEAD_DIM, MODEL_DIM), 1.5 * (HEADS * HEAD_DIM) ** -0.5),
        "mlp_norm": gain_vector(shared[5]),
        "w_gate": normal_weight(shared[6], (MODEL_DIM, FFN_DIM), MODEL_DIM ** -0.5),
        "w_up": normal_weight(shared[7], (MODEL_DIM, FFN_DIM), MODEL_DIM ** -0.5),
        "w_down": normal_weight(shared[8], (FFN_DIM, MODEL_DIM), 1.5 * FFN_DIM ** -0.5),
        "final_norm": gain_vector(shared[9]),
        "w_lm": normal_weight(shared[10], (MODEL_DIM, VOCAB_SIZE), 3.0 * MODEL_DIM ** -0.5),
    }


def rms_norm(values, gain):
    widened = values.astype(jnp.float32)
    scale = lax.rsqrt(jnp.mean(widened * widened, axis=-1, keepdims=True) + RMS_EPS)
    return (widened * scale * gain.astype(jnp.float32)).astype(jnp.bfloat16)


def rotate(values, positions):
    head_dim = values.shape[-1]
    half = head_dim // 2
    inv_freq = 1.0 / (ROPE_THETA ** (jnp.arange(half, dtype=jnp.float32) * (2.0 / head_dim)))
    angles = positions.astype(jnp.float32)[..., None] * inv_freq
    cosine = jnp.cos(angles)[..., None, :]
    sine = jnp.sin(angles)[..., None, :]
    first = values[..., :half]
    second = values[..., half:]
    return jnp.concatenate([first * cosine - second * sine, second * cosine + first * sine], axis=-1)


def reference(hidden, tree_mask, depth, ctx_len, block_table, score_id, k_cache, v_cache, attn_norm, w_q, w_k, w_v, w_o, mlp_norm, w_gate, w_up, w_down, final_norm, w_lm):
    scale = HEAD_DIM ** -0.5
    slot_ids = jnp.arange(SPAN)

    def one_request(item):
        rows, mask_row, depth_row, context, table_row, targets = item
        normed = rms_norm(rows, attn_norm)
        positions = context + depth_row
        query = jnp.dot(normed, w_q, preferred_element_type=jnp.float32).reshape(NODES, HEADS, HEAD_DIM)
        query = rotate(query, positions).astype(jnp.bfloat16).reshape(NODES, KV_HEADS, GROUP, HEAD_DIM)
        key_new = jnp.dot(normed, w_k, preferred_element_type=jnp.float32).reshape(NODES, KV_HEADS, HEAD_DIM)
        key_new = rotate(key_new, positions).astype(jnp.bfloat16)
        val_new = jnp.dot(normed, w_v, preferred_element_type=jnp.float32).astype(jnp.bfloat16).reshape(NODES, KV_HEADS, HEAD_DIM)
        key_old = k_cache[table_row].reshape(SPAN, KV_HEADS, HEAD_DIM)
        val_old = v_cache[table_row].reshape(SPAN, KV_HEADS, HEAD_DIM)
        query_wide = query.astype(jnp.float32)
        score_old = jnp.einsum("tkgh,skh->tkgs", query_wide, key_old.astype(jnp.float32)) * scale
        score_old = jnp.where((slot_ids < context)[None, None, None, :], score_old, -jnp.inf)
        score_new = jnp.einsum("tkgh,jkh->tkgj", query_wide, key_new.astype(jnp.float32)) * scale
        score_new = jnp.where((mask_row > 0)[:, None, None, :], score_new, -jnp.inf)
        top = jnp.maximum(jnp.max(score_old, axis=-1), jnp.max(score_new, axis=-1))[..., None]
        prob_old = jnp.exp(score_old - top)
        prob_new = jnp.exp(score_new - top)
        total = jnp.sum(prob_old, axis=-1) + jnp.sum(prob_new, axis=-1)
        mixed = jnp.einsum("tkgs,skh->tkgh", prob_old.astype(jnp.bfloat16).astype(jnp.float32), val_old.astype(jnp.float32))
        mixed = mixed + jnp.einsum("tkgj,jkh->tkgh", prob_new.astype(jnp.bfloat16).astype(jnp.float32), val_new.astype(jnp.float32))
        attended = (mixed / total[..., None]).astype(jnp.bfloat16).reshape(NODES, HEADS * HEAD_DIM)
        attn_out = jnp.dot(attended, w_o, preferred_element_type=jnp.float32).astype(jnp.bfloat16)
        residual = (rows.astype(jnp.float32) + attn_out.astype(jnp.float32)).astype(jnp.bfloat16)
        normed_mlp = rms_norm(residual, mlp_norm)
        gate = jnp.dot(normed_mlp, w_gate, preferred_element_type=jnp.float32)
        upper = jnp.dot(normed_mlp, w_up, preferred_element_type=jnp.float32)
        product = (jax.nn.silu(gate) * upper).astype(jnp.bfloat16)
        mlp_out = jnp.dot(product, w_down, preferred_element_type=jnp.float32).astype(jnp.bfloat16)
        layer_out = (residual.astype(jnp.float32) + mlp_out.astype(jnp.float32)).astype(jnp.bfloat16)
        logits = jnp.dot(rms_norm(layer_out, final_norm), w_lm, preferred_element_type=jnp.float32)
        log_norm = jax.nn.logsumexp(logits, axis=-1)
        picked = jnp.take_along_axis(logits, targets[:, None], axis=-1)[:, 0]
        return log_norm, picked - log_norm, key_new, val_new

    log_norm, log_prob, key_new, val_new = lax.map(one_request, (hidden, tree_mask, depth, ctx_len, block_table, score_id))
    slots = ctx_len[:, None] + jnp.arange(NODES)[None, :]
    slot_blocks = jnp.take_along_axis(block_table, slots // PAGE_SIZE, axis=1)
    k_out = k_cache.at[slot_blocks, slots % PAGE_SIZE].set(key_new)
    v_out = v_cache.at[slot_blocks, slots % PAGE_SIZE].set(val_new)
    return (log_norm, log_prob, k_out, v_out)
```

```python
import functools

import jax
import jax.numpy as jnp
import numpy as np
from jax import lax
from jax.experimental import pallas as pl
from jax.experimental.pallas import tpu as pltpu
from jax.sharding import PartitionSpec as P

RMS_EPS = 1e-5
ROPE_THETA = 500000
NEG = -1e30
CHUNKS = 4
SLOTS = 3
F32 = jnp.float32
BF16 = jnp.bfloat16


def dot(a, b):
    return lax.dot_general(a, b, (((1,), (0,)), ((), ())), preferred_element_type=F32)


def dot_t(a, b):
    return lax.dot_general(a, b, (((1,), (1,)), ((), ())), preferred_element_type=F32)


def iota(shape, axis):
    return lax.broadcasted_iota(jnp.int32, shape, axis)


def attention_kernel(dims, ctx_ref, table_ref, mask_ref, freq_ref, gain_ref, hid_hbm, wq_hbm, wk_hbm, wv_hbm, kc_hbm, vc_hbm, att_ref, ko_hbm, vo_hbm, hid, wq, wk, wv, kc, vc, normed, sumsq, in_sem, out_sem):
    requests, nodes, pages, page = dims
    rows, width = hid.shape
    head_dim = freq_ref.shape[1]
    heads = wq.shape[1] // head_dim
    pairs = [(hid_hbm, hid), (wq_hbm, wq), (wk_hbm, wk), (kc_hbm, kc), (wv_hbm, wv), (vc_hbm, vc)]
    copies = [pltpu.make_async_copy(src, dst, in_sem.at[i]) for i, (src, dst) in enumerate(pairs)]
    for copy in copies:
        copy.start()

    tree = mask_ref[...]
    depth = jnp.sum(tree, axis=1, keepdims=True) - 1
    position = jnp.concatenate([depth[b * nodes : (b + 1) * nodes] + ctx_ref[b] for b in range(requests)], axis=0)
    angle = position.astype(F32) * freq_ref[...]
    cosine = jnp.cos(angle)
    sine = jnp.sin(angle)
    sine = jnp.where(iota(sine.shape, 1) < head_dim // 2, -sine, sine)

    copies[0].wait()
    step = 32

    def square(i, carry):
        at = pl.ds(pl.multiple_of(i * step, step), step)
        total = jnp.zeros((step, 128), F32)
        for j in range(width // 512):
            x = hid[at, j * 512 : (j + 1) * 512].astype(F32)
            x = x * x
            total = total + ((x[:, :128] + x[:, 128:256]) + (x[:, 256:384] + x[:, 384:]))
        sumsq[at, :] = total
        return carry

    lax.fori_loop(0, rows // step, square, 0)
    scale = lax.rsqrt(jnp.sum(sumsq[...], axis=1, keepdims=True) * (1.0 / width) + RMS_EPS)
    sumsq[...] = jnp.broadcast_to(scale, sumsq.shape)

    def apply(i, carry):
        at = pl.ds(pl.multiple_of(i * step, step), step)
        s = sumsq[at, :]
        s = jnp.concatenate([s] * 4, axis=1)
        for j in range(width // 512):
            cols = slice(j * 512, (j + 1) * 512)
            normed[at, cols] = (hid[at, cols].astype(F32) * s * gain_ref[:, cols]).astype(BF16)
        return carry

    lax.fori_loop(0, rows // step, apply, 0)

    def rotate(x):
        return (x * cosine + pltpu.roll(x, head_dim // 2, 1) * sine).astype(BF16)

    def by_head(x):
        return [x[:, h * head_dim : (h + 1) * head_dim] for h in range(heads)]

    copies[1].wait()
    query = [rotate(x) for x in by_head(dot(normed[...], wq[...]))]
    copies[2].wait()
    key_new = [rotate(x) for x in by_head(dot(normed[...], wk[...]))]
    copies[4].wait()
    val_new = [x.astype(BF16) for x in by_head(dot(normed[...], wv[...]))]

    def stack(parts, b):
        return jnp.concatenate([x[b * nodes : (b + 1) * nodes] for x in parts], axis=0)

    queries = [stack(query, b) for b in range(requests)]
    keys = [stack(key_new, b) for b in range(requests)]
    vals = [stack(val_new, b) for b in range(requests)]

    copies[3].wait()
    copies[5].wait()
    n_pages = nodes // page + 1
    wide = page * heads
    for b in range(requests):
        ctx = ctx_ref[b]
        first = ctx // page
        off = ctx - first * page
        r = iota((n_pages * wide, heads * nodes), 0)
        c = iota((n_pages * wide, heads * nodes), 1)
        j = r // heads - off
        pick = (j >= 0) & (j < nodes) & (c == (r % heads) * nodes + j)
        onehot = jnp.where(pick, 1.0, 0.0).astype(BF16)
        for cache, new in ((kc, keys[b]), (vc, vals[b])):
            window = dot(onehot, new)
            for p in range(n_pages):
                block = table_ref[b, jnp.minimum(first + p, pages - 1)]
                slot = iota((wide, head_dim), 0) // heads + (p * page) - off
                old = cache[block].astype(F32)
                cache[block] = jnp.where((slot >= 0) & (slot < nodes), window[p * wide : (p + 1) * wide], old).astype(BF16)
    outs = [pltpu.make_async_copy(kc, ko_hbm, out_sem.at[0]), pltpu.make_async_copy(vc, vo_hbm, out_sem.at[1])]
    for copy in outs:
        copy.start()

    span = pages * wide
    many = heads * nodes
    factor = head_dim**-0.5
    same_old = iota((many, span), 1) % heads == iota((many, span), 0) // nodes
    slot_old = iota((many, span), 1) // heads
    same_new = iota((many, many), 1) // nodes == iota((many, many), 0) // nodes
    old_scores, new_scores = [], []
    for b in range(requests):
        k_old = jnp.concatenate([kc[table_ref[b, p]] for p in range(pages)], axis=0)
        s_old = dot_t(queries[b], k_old) * factor
        old_scores.append(jnp.where(same_old & (slot_old < ctx_ref[b]), s_old, NEG))
        seen = tree[b * nodes : (b + 1) * nodes]
        seen = jnp.concatenate([seen] * heads, axis=1)
        seen = jnp.concatenate([seen] * heads, axis=0)
        s_new = dot_t(queries[b], keys[b]) * factor
        new_scores.append(jnp.where(same_new & (seen > 0), s_new, NEG))
    for b in range(requests):
        top = jnp.maximum(jnp.max(old_scores[b], axis=1, keepdims=True), jnp.max(new_scores[b], axis=1, keepdims=True))
        p_old = jnp.exp(old_scores[b] - top)
        p_new = jnp.exp(new_scores[b] - top)
        total = jnp.sum(p_old, axis=1, keepdims=True) + jnp.sum(p_new, axis=1, keepdims=True)
        v_old = jnp.concatenate([vc[table_ref[b, p]] for p in range(pages)], axis=0)
        mixed = dot(p_old.astype(BF16), v_old) + dot(p_new.astype(BF16), vals[b])
        mixed = (mixed / total).astype(BF16)
        for h in range(heads):
            att_ref[b * nodes : (b + 1) * nodes, h * head_dim : (h + 1) * head_dim] = mixed[h * nodes : (h + 1) * nodes]
    for copy in outs:
        copy.wait()


def attention(hidden, tree_mask, ctx_len, block_table, k_cache, v_cache, attn_norm, w_q, w_k, w_v):
    requests, nodes, width = hidden.shape
    blocks, page, heads, head_dim = k_cache.shape
    pages = block_table.shape[1]
    rows = requests * nodes
    half = head_dim // 2
    inv_freq = 1.0 / (np.float32(ROPE_THETA) ** (np.arange(half, dtype=np.float32) * np.float32(2.0 / head_dim)))
    freq = jnp.asarray(np.concatenate([inv_freq, inv_freq])[None].astype(np.float32))
    pages_shape = (blocks, page * heads, head_dim)
    vmem = pl.BlockSpec(memory_space=pltpu.VMEM)
    smem = pl.BlockSpec(memory_space=pltpu.SMEM)
    hbm = pl.BlockSpec(memory_space=pl.ANY)
    cache = jax.ShapeDtypeStruct(pages_shape, BF16)
    local = w_q.shape[1]
    att, k_out, v_out = pl.pallas_call(
        functools.partial(attention_kernel, (requests, nodes, pages, page)),
        name="tree_attention",
        out_shape=(jax.ShapeDtypeStruct((rows, local), BF16), cache, cache),
        in_specs=[smem, smem, vmem, vmem, vmem] + [hbm] * 6,
        out_specs=(vmem, hbm, hbm),
        scratch_shapes=[
            pltpu.VMEM((rows, width), BF16),
            pltpu.VMEM((width, local), BF16),
            pltpu.VMEM((width, local), BF16),
            pltpu.VMEM((width, local), BF16),
            pltpu.VMEM(pages_shape, BF16),
            pltpu.VMEM(pages_shape, BF16),
            pltpu.VMEM((rows, width), BF16),
            pltpu.VMEM((rows, 128), F32),
            pltpu.SemaphoreType.DMA((6,)),
            pltpu.SemaphoreType.DMA((2,)),
        ],
        compiler_params=pltpu.CompilerParams(vmem_limit_bytes=67043328),
    )(
        ctx_len,
        block_table,
        tree_mask.reshape(rows, nodes),
        freq,
        attn_norm.astype(F32)[None],
        hidden.reshape(rows, width),
        w_q,
        w_k,
        w_v,
        k_cache.reshape(pages_shape),
        v_cache.reshape(pages_shape),
    )
    return att, k_out.reshape(k_cache.shape), v_out.reshape(v_cache.shape)


def layer_kernel(n, ids_ref, gm_ref, gf_ref, att_hbm, hid_hbm, wo_hbm, wg_hbm, wu_hbm, wd_hbm, wlm_hbm, ln_ref, lp_ref, *scratch):
    (
        att, hid, wo, wg, wu, wd, wlm, acc, gate, up, prod, xn, scale_ref, own, d2d_send, d2d_recv, rs_send, rs_recv, mine, part,
        ssq_send, ssq_recv, st_send, st_recv, lanes,
        load_sem, lm_sem, pair_sems, pair_recv, rs_sems, rs_rsem, ag_sems, ag_rsem, hp_sems, hp_rsem, sq_sems, sq_rsem, st_sems, st_rsem,
    ) = scratch
    chips = n // 2
    far = chips // 2
    rows, cb = hid.shape
    rc = rows // CHUNKS
    half = CHUNKS // 2
    width = cb * n
    me = lax.axis_index("tp")
    z, c = me // 2, me % 2
    partner = z * 2 + (1 - c)
    ring = (lax.rem(z + 1, chips) * 2 + c, lax.rem(z + chips - 1, chips) * 2 + c)

    def remote(src, dst, send, recv, device):
        return pltpu.make_async_remote_copy(
            src_ref=src, dst_ref=dst, send_sem=send, recv_sem=recv, device_id={"tp": device}, device_id_type=pl.DeviceIdType.MESH
        )

    sent = []

    def start(copy):
        copy.start()
        sent.append(copy)

    def drain():
        while sent:
            sent.pop(0).wait_send()

    def chip_at(offset):
        return lax.rem(z + offset, chips)

    loads = [
        pltpu.make_async_copy(src, dst, load_sem.at[i])
        for i, (src, dst) in enumerate(
            [
                (att_hbm, att),
                (wo_hbm, wo),
                (hid_hbm.at[:, pl.ds(pl.multiple_of(me * cb, cb), cb)], hid),
                (wg_hbm, wg),
                (wu_hbm, wu),
                (wd_hbm, wd),
            ]
        )
    ]
    for copy in loads[:3]:
        copy.start()
    barrier = pltpu.get_barrier_semaphore()
    for k in range(1, n):
        pl.semaphore_signal(barrier, inc=1, device_id={"tp": lax.rem(me + k, n)}, device_id_type=pl.DeviceIdType.MESH)
    pl.semaphore_wait(barrier, n - 1)
    for copy in loads[3:]:
        copy.start()

    consume = [0]
    for d in range(1, far):
        consume += [chips - d, d]
    consume += [far]

    def lm_load(j):
        at = pl.multiple_of(chip_at(consume[j]) * (2 * cb), 2 * cb)
        return pltpu.make_async_copy(wlm_hbm.at[pl.ds(at, 2 * cb)], wlm.at[j % SLOTS], lm_sem.at[j % SLOTS])

    for j in range(SLOTS):
        lm_load(j).start()

    order = [far]
    for d in range(far - 1, 0, -1):
        order += [d, chips - d]
    order += [0]

    def reduce_scatter(ph, lhs, weight):
        waited = set()

        def compute(i):
            base = chip_at(order[i]) * (2 * cb)
            other = pl.ds(pl.multiple_of(base + (1 - c) * cb, cb), cb)
            d2d_send[i] = dot(lhs, weight[:, other]).astype(BF16)
            start(remote(d2d_send.at[i], d2d_recv.at[ph, i], pair_sems.at[i], pair_recv.at[ph, i], partner))
            own[i] = dot(lhs, weight[:, pl.ds(pl.multiple_of(base + c * cb, cb), cb)])

        def local(i, k):
            if i not in waited:
                waited.add(i)
                remote(d2d_send.at[i], d2d_recv.at[ph, i], pair_sems.at[i], pair_recv.at[ph, i], partner).wait_recv()
            at = slice(k * rc, (k + 1) * rc)
            return own[i, at, :] + d2d_recv[ph, i, at, :].astype(F32)

        def unit(way, d, k):
            return remote(rs_send.at[way, d - 1, k], rs_recv.at[ph, way, d - 1, k], rs_sems.at[way, d - 1, k], rs_rsem.at[ph, way, d - 1, k], ring[way])

        def far_half(way):
            return range(half) if way == 0 else range(half, CHUNKS)

        def near_half(way):
            return range(half, CHUNKS) if way == 0 else range(half)

        def hop(d):
            for part_of in (near_half, far_half):
                if d == far and part_of is near_half:
                    continue
                for q in range(half):
                    for way in (0, 1):
                        k = part_of(way)[q]
                        i = order.index(d if way == 0 else chips - d)
                        value = local(i, k)
                        if d + 1 < far or (d + 1 == far and k in far_half(way)):
                            unit(way, d + 1, k).wait_recv()
                            value = value + rs_recv[ph, way, d, k].astype(F32)
                        rs_send[way, d - 1, k] = value.astype(BF16)
                        start(unit(way, d, k))

        compute(0)
        done = 1
        for d in range(far, 0, -1):
            ahead = 2 if d > 1 else 1
            for _ in range(ahead):
                if done < chips:
                    compute(done)
                    done += 1
            hop(d)
        while done < chips:
            compute(done)
            done += 1
        sums = []
        last = order.index(0)
        for k in range(CHUNKS):
            value = local(last, k)
            for way in (0, 1):
                unit(way, 1, k).wait_recv()
                value = value + rs_recv[ph, way, 0, k].astype(F32)
            sums.append(value.astype(BF16))
        return sums

    def broadcast_sumsq(ph, squares):
        ssq_send[...] = jnp.sum(jnp.transpose(squares), axis=0, keepdims=True)
        ssq_recv[ph, me] = ssq_send[...]
        for k in range(1, n):
            start(remote(ssq_send, ssq_recv.at[ph, me], sq_sems.at[k], sq_rsem.at[ph, me], lax.rem(me + k, n)))

    def wait_scale(ph):
        for k in range(1, n):
            src = lax.rem(me + k, n)
            remote(ssq_send, ssq_recv.at[ph, src], sq_sems.at[k], sq_rsem.at[ph, src], src).wait_recv()
        total = ssq_recv[ph, 0]
        for j in range(1, n):
            total = total + ssq_recv[ph, j]
        scale = lax.rsqrt(total * (1.0 / width) + RMS_EPS)
        scale_ref[...] = jnp.transpose(jnp.broadcast_to(scale, (128, rows)))

    def residual_gather(ph, sums, before, gain_ref, block):
        squares = jnp.zeros((rows, 128), F32)
        wides = []
        for k in range(CHUNKS):
            at = slice(k * rc, (k + 1) * rc)
            value = (before[at, :].astype(F32) + sums[k].astype(F32)).astype(BF16)
            mine[ph, 0, at, :] = value
            value = value.astype(F32)
            value = value * value
            total = value[:, :128]
            for i in range(1, cb // 128):
                total = total + value[:, i * 128 : (i + 1) * 128]
            wides.append(total)
        squares = jnp.concatenate(wides, axis=0)
        broadcast_sumsq(ph, squares)

        def hop(way, r, k):
            to = (r - 1) % chips if way == 0 else (r + 1) % chips
            at = pl.ds(k * rc, rc)
            return remote(mine.at[ph, r, at], mine.at[ph, to, at], ag_sems.at[way, r, k], ag_rsem.at[ph, to, k], ring[way])

        def arrive(way, r, k):
            at = pl.ds(k * rc, rc)
            back = (r + 1) % chips if way == 0 else (r - 1) % chips
            remote(mine.at[ph, back, at], mine.at[ph, r, at], ag_sems.at[way, back, k], ag_rsem.at[ph, r, k], ring[way]).wait_recv()

        def across(r):
            return remote(mine.at[ph, r], part.at[ph, r], hp_sems.at[r], hp_rsem.at[ph, r], partner)

        for q in range(half):
            for way in (0, 1):
                start(hop(way, 0, q if way == 0 else half + q))
        for q in range(half):
            for way in (0, 1):
                start(hop(way, 0, half + q if way == 0 else q))
        start(across(0))

        def forward(d):
            for part_of in (0, 1):
                for q in range(half):
                    for way in (0, 1):
                        r = chips - d if way == 0 else d
                        far_chunk = part_of == 0
                        k = q if (way == 0) == far_chunk else half + q
                        if d == far and not far_chunk:
                            continue
                        arrive(way, r, k)
                        if d + 1 < far or (d + 1 == far and far_chunk):
                            start(hop(way, r, k))
            start(across(d))
            if d != far:
                start(across(chips - d))

        def process(j):
            r = consume[j]
            across(r).wait_recv()
            t = chip_at(r)
            s = scale_ref[...]
            s = jnp.concatenate([s] * (cb // 128), axis=1)
            xn[c] = (mine[ph, r].astype(F32) * s * gain_ref[t * 2 + c]).astype(BF16)
            xn[1 - c] = (part[ph, r].astype(F32) * s * gain_ref[t * 2 + 1 - c]).astype(BF16)
            block(j, t, jnp.concatenate([xn[0], xn[1]], axis=1))

        forward(1)
        wait_scale(ph)
        process(0)
        todo = 1
        for d in range(2, far + 1):
            process(todo)
            forward(d)
            process(todo + 1)
            todo += 2
        while todo < chips:
            process(todo)
            todo += 1

    loads[0].wait()
    loads[1].wait()
    sums = reduce_scatter(0, att[...], wo)
    loads[2].wait()
    drain()
    loads[3].wait()
    loads[4].wait()

    def mlp_block(j, t, x):
        at = pl.ds(pl.multiple_of(t * (2 * cb), 2 * cb), 2 * cb)
        g = dot_t(x, wg[:, at])
        u = dot_t(x, wu[:, at])
        if j == 0:
            gate[...] = g
            up[...] = u
        elif j < chips - 1:
            gate[...] += g
            up[...] += u
        else:
            g = gate[...] + g
            prod[...] = (g * jax.nn.sigmoid(g) * (up[...] + u)).astype(BF16)

    residual_gather(0, sums, hid, gm_ref, mlp_block)
    drain()
    loads[5].wait()
    sums = reduce_scatter(1, prod[...], wd)
    drain()

    cols = acc.shape[1]
    tiles = 2 if cols % 256 == 0 else 1
    tile = cols // tiles

    def head_block(j, t, x):
        lm_load(j).wait()
        slot = j % SLOTS

        def piece(i, carry):
            at = pl.ds(pl.multiple_of(i * tile, tile), tile)
            y = dot(x, wlm[slot, :, at])
            if j == 0:
                acc[:, at] = y
            else:
                acc[:, at] += y
            return carry

        lax.fori_loop(0, tiles, piece, 0)
        if j + SLOTS < chips:
            lm_load(j + SLOTS).start()

    residual_gather(1, sums, mine.at[0, 0], gf_ref, head_block)

    wanted = jnp.transpose(jnp.broadcast_to((ids_ref[...] - me * cols).astype(F32), (128, rows)))
    lanes[3] = wanted
    block = 64

    def stats(i, carry):
        at = pl.ds(pl.multiple_of(i * block, block), block)
        top = acc[at, 0:128]
        for j in range(1, cols // 128):
            top = jnp.maximum(top, acc[at, j * 128 : (j + 1) * 128])
        want = lanes[3, at, :] - iota((block, 128), 1).astype(F32)
        total = jnp.zeros((block, 128), F32)
        picked = jnp.zeros((block, 128), F32)
        for j in range(cols // 128):
            x = acc[at, j * 128 : (j + 1) * 128]
            total = total + jnp.exp(x - top)
            picked = picked + jnp.where(want == float(j * 128), x, 0.0)
        lanes[0, at, :] = top
        lanes[1, at, :] = total
        lanes[2, at, :] = picked
        return carry

    lax.fori_loop(0, rows // block, stats, 0)
    top = jnp.transpose(lanes[0])
    total = jnp.transpose(lanes[1])
    high = jnp.max(top, axis=0, keepdims=True)
    total = jnp.sum(total * jnp.exp(top - high), axis=0, keepdims=True)
    st_send[0:1] = high + jnp.log(total)
    st_send[1:2] = jnp.sum(jnp.transpose(lanes[2]), axis=0, keepdims=True)
    st_recv[me] = st_send[...]
    for k in range(1, n):
        start(remote(st_send, st_recv.at[me], st_sems.at[k], st_rsem.at[me], lax.rem(me + k, n)))
    for k in range(1, n):
        src = lax.rem(me + k, n)
        remote(st_send, st_recv.at[src], st_sems.at[k], st_rsem.at[src], src).wait_recv()
    every = [st_recv[j] for j in range(n)]
    high = every[0][0:1]
    for x in every[1:]:
        high = jnp.maximum(high, x[0:1])
    total = jnp.zeros_like(high)
    picked = jnp.zeros_like(high)
    for x in every:
        total = total + jnp.exp(x[0:1] - high)
        picked = picked + x[1:2]
    log_norm = high + jnp.log(total)
    ln_ref[...] = log_norm
    lp_ref[...] = picked - log_norm
    drain()


def layer_and_head(n, att, hidden, score_id, w_o, mlp_norm, w_gate, w_up, w_down, final_norm, w_lm):
    requests, nodes, width = hidden.shape
    rows = requests * nodes
    cb = width // n
    chips = n // 2
    rc = rows // CHUNKS
    ffn = w_gate.shape[1]
    cols = w_lm.shape[1]
    vmem = pl.BlockSpec(memory_space=pltpu.VMEM)
    hbm = pl.BlockSpec(memory_space=pl.ANY)
    dma = pltpu.SemaphoreType.DMA
    row = jax.ShapeDtypeStruct((1, rows), F32)
    log_norm, log_prob = pl.pallas_call(
        functools.partial(layer_kernel, n),
        name="layer_and_head",
        out_shape=(row, row),
        in_specs=[vmem] * 3 + [hbm] * 7,
        out_specs=(vmem, vmem),
        scratch_shapes=[
            pltpu.VMEM(att.shape, BF16),
            pltpu.VMEM((rows, cb), BF16),
            pltpu.VMEM(w_o.shape, BF16),
            pltpu.VMEM((ffn, width), BF16),
            pltpu.VMEM((ffn, width), BF16),
            pltpu.VMEM((ffn, width), BF16),
            pltpu.VMEM((SLOTS, 2 * cb, cols), BF16),
            pltpu.VMEM((rows, cols), F32),
            pltpu.VMEM((rows, ffn), F32),
            pltpu.VMEM((rows, ffn), F32),
            pltpu.VMEM((rows, ffn), BF16),
            pltpu.VMEM((2, rows, cb), BF16),
            pltpu.VMEM((rows, 128), F32),
            pltpu.VMEM((chips, rows, cb), F32),
            pltpu.VMEM((chips, rows, cb), BF16),
            pltpu.VMEM((2, chips, rows, cb), BF16),
            pltpu.VMEM((2, chips // 2, CHUNKS, rc, cb), BF16),
            pltpu.VMEM((2, 2, chips // 2, CHUNKS, rc, cb), BF16),
            pltpu.VMEM((2, chips, rows, cb), BF16),
            pltpu.VMEM((2, chips, rows, cb), BF16),
            pltpu.VMEM((1, rows), F32),
            pltpu.VMEM((2, n, 1, rows), F32),
            pltpu.VMEM((2, rows), F32),
            pltpu.VMEM((n, 2, rows), F32),
            pltpu.VMEM((4, rows, 128), F32),
            dma((6,)),
            dma((SLOTS,)),
            dma((chips,)),
            dma((2, chips)),
            dma((2, chips // 2, CHUNKS)),
            dma((2, 2, chips // 2, CHUNKS)),
            dma((2, chips, CHUNKS)),
            dma((2, chips, CHUNKS)),
            dma((chips,)),
            dma((2, chips)),
            dma((n,)),
            dma((2, n)),
            dma((n,)),
            dma((n,)),
        ],
        compiler_params=pltpu.CompilerParams(collective_id=0, has_side_effects=True, vmem_limit_bytes=67043328),
    )(
        score_id.reshape(1, rows),
        mlp_norm.astype(F32).reshape(n, 1, cb),
        final_norm.astype(F32).reshape(n, 1, cb),
        att,
        hidden.reshape(rows, width),
        w_o,
        w_gate.T,
        w_up.T,
        w_down,
        w_lm,
    )
    return log_norm.reshape(requests, nodes), log_prob.reshape(requests, nodes)


def solution(mesh):
    n = mesh.shape["tp"]

    def group_step(hidden, tree_mask, depth, ctx_len, block_table, score_id, k_cache, v_cache, attn_norm, w_q, w_k, w_v, w_o, mlp_norm, w_gate, w_up, w_down, final_norm, w_lm):
        att, k_out, v_out = attention(hidden, tree_mask, ctx_len, block_table, k_cache, v_cache, attn_norm, w_q, w_k, w_v)
        log_norm, log_prob = layer_and_head(n, att, hidden, score_id, w_o, mlp_norm, w_gate, w_up, w_down, final_norm, w_lm)
        return log_norm, log_prob, k_out, v_out

    request_spec = P("dp", None, None)
    node_spec = P("dp", None)
    cache_spec = P("dp", None, "tp", None)
    shared_spec = P(None)
    column_spec = P(None, "tp")
    row_spec = P("tp", None)
    in_specs = (request_spec, request_spec, node_spec, P("dp"), node_spec, node_spec, cache_spec, cache_spec, shared_spec, column_spec, column_spec, column_spec, row_spec, shared_spec, column_spec, column_spec, row_spec, shared_spec, column_spec)
    out_specs = (node_spec, node_spec, cache_spec, cache_spec)
    return jax.shard_map(group_step, mesh=mesh, in_specs=in_specs, out_specs=out_specs, check_vma=False)
```
